256 devices in a mesh: dp: 8 (over z), expert: 32 (over x, y, core).
Axes of the slice: x: 4, y: 4, z: 8, core: 2. Of those that a mesh axis runs over, the one named last changes fastest.
Arguments:
- tokens: bfloat16 [65536, 2048], P(('dp', 'expert')), may hold values from -6 to 6
- expert_ranks: int32 [32, 65536], P(None, ('dp', 'expert')), may hold values from 0 to 65535, as said below
- capacity: int32 [32], replicated, may hold values from 512 to 1024, as said below
- weight_in: bfloat16 [32, 2048, 8192], P('expert', None, 'dp'), may hold values from -0.125 to 0.125
- weight_out: bfloat16 [32, 8192, 2048], P('expert', 'dp'), may hold values from -0.0625 to 0.0625
- gate_weights: float32 [32, 1024], P('expert', 'dp'), may hold values from 0.05 to 1
Outputs:
- combined: bfloat16 [65536, 2048], P(('dp', 'expert'))
The draws below stay inside these ranges and needn't reach their ends.
Inputs may be any that keep to these rules, and one draw needn't show every extreme that they name: `expert_ranks`: for each expert the ranks are a permutation of 0 to 65535. Of the 256 tokens of one device, at most 8 have rank under 1024 for one expert; for an expert of capacity 1024, some devices have exactly 8. At least one expert has capacity 1024.
All inputs are finite; a program needn't handle non-finite values.
Results may differ from the reference program's by a relative error of at most 0.0053.
Values may be sent and summed in bfloat16 or wider, within the bound.
A program may use at most 64 MiB of HBM per device.

```python
import math
import jax
import jax.numpy as jnp
from jax import lax

D = 2048
FF = 8192
TOK_DEV = 256
EXPERTS = 32
TOKENS = 65536
CAP = 1024


def local_permutation(subkey):
    return jax.random.permutation(subkey, TOK_DEV)


def device_permutation(subkey):
    return jax.random.permutation(subkey, TOKENS // TOK_DEV)


def token_permutation(subkey):
    return jax.random.permutation(subkey, TOKENS)


def draw_expert_ranks(key, part):
    devices_all = TOKENS // TOK_DEV
    average = TOK_DEV // 64
    low_total = 3 * average // 2
    key_mid = jax.random.fold_in(key, 11)
    key_low = jax.random.fold_in(key, 12)
    key_order = jax.random.fold_in(key, 13)
    key_local = jax.random.fold_in(key, 14)
    key_ties = jax.random.fold_in(key, 15)
    position = lax.broadcasted_iota(jnp.int32, (EXPERTS, devices_all), 1)
    paired = position // 2
    leading = position % 2 == 0
    middle_draw = jax.random.randint(key_mid, (EXPERTS, devices_all // 2), average // 2, average + average // 2 + 1)
    low_draw = jax.random.randint(key_low, (EXPERTS, devices_all // 2), average // 4, low_total - average // 4 + 1)
    middle_pick = jnp.take_along_axis(middle_draw, paired, axis=1)
    low_pick = jnp.take_along_axis(low_draw, paired, axis=1)
    middle_value = jnp.where(leading, middle_pick, 2 * average - middle_pick)
    low_value = jnp.where(leading, low_pick, low_total - low_pick)
    pattern = jnp.where(position < devices_all // 8, 2 * average, jnp.where(position < devices_all // 2, middle_value, low_value))
    orders = jax.vmap(device_permutation)(jax.random.split(key_order, EXPERTS))
    quota = jnp.take_along_axis(pattern, orders, axis=1).astype(jnp.int32)
    locals_all = jax.vmap(local_permutation)(jax.random.split(key_local, EXPERTS * devices_all))
    locals_all = locals_all.reshape(EXPERTS, devices_all, TOK_DEV)
    selected = (locals_all < quota[:, :, None]).reshape(EXPERTS, TOKENS)
    ties = jax.vmap(token_permutation)(jax.random.split(key_ties, EXPERTS)).astype(jnp.int32)
    score = jnp.where(selected, ties, TOKENS + ties).astype(jnp.int32)
    order = jnp.argsort(score, axis=1, stable=True)
    ranks = jnp.argsort(order, axis=1, stable=True)
    return ranks.astype(jnp.int32)


def draw_capacity(key, part):
    key_values = jax.random.fold_in(key, 21)
    key_full = jax.random.fold_in(key, 22)
    values = jax.random.randint(key_values, (EXPERTS,), CAP // 2, CAP + 1)
    full_index = jax.random.randint(key_full, (), 0, EXPERTS)
    position = lax.broadcasted_iota(jnp.int32, (EXPERTS,), 0)
    return jnp.where(position == full_index, CAP, values).astype(jnp.int32)


def shard_levels(key, shape, cuts, smallest, top_value):
    loudness = 1.0
    for axis_at, parts in cuts:
        steps = jax.random.uniform(jax.random.fold_in(jax.random.fold_in(key, 6), axis_at), (parts,), jnp.float32, smallest / len(cuts), top_value / len(cuts))
        loudness = loudness * jnp.repeat(jnp.exp(steps), shape[axis_at] // parts).reshape((-1,) + (1,) * (len(shape) - 1 - axis_at))
    return loudness


def gaussian(stream_key, shape, width, most, cuts=(), kind=jnp.bfloat16):
    result = jax.random.normal(stream_key, shape, jnp.float32) * width
    if len(cuts) > 0:
        result = shard_levels(stream_key, shape, cuts, -0.22, 0.18) * result
    return jnp.clip(result, min=-most, max=most).astype(kind)


def setup_inputs(seed: int = 0) -> dict:
    key_list = jax.random.split(jax.random.key(seed), 7)
    tokens = gaussian(key_list[0], (TOKENS, D), 1.0, 6.0, ((0, 256),))
    expert_ranks = draw_expert_ranks(jax.random.fold_in(key_list[6], 71), 0)
    capacity = draw_capacity(jax.random.fold_in(key_list[6], 71), 0)
    weight_in = gaussian(key_list[3], (EXPERTS, D, FF), D ** -0.5, 0.125, ((0, 32), (2, 8)))
    weight_out = gaussian(key_list[4], (EXPERTS, FF, D), FF ** -0.5, 0.0625, ((0, 32), (1, 8)))
    gate_weights = jnp.clip(jnp.exp(math.log(1.0) - 2.9957323 * jax.random.uniform(key_list[5], (EXPERTS, CAP), jnp.float32) ** shard_levels(key_list[5], (EXPERTS, CAP), ((0, 32), (1, 8)), -0.2, 0.2)), 0.05, 1.0)
    return {"tokens": tokens, "expert_ranks": expert_ranks, "capacity": capacity, "weight_in": weight_in, "weight_out": weight_out, "gate_weights": gate_weights}


def reference(tokens, expert_ranks, capacity, weight_in, weight_out, gate_weights):
    total = tokens.shape[0]
    tokens_wide = tokens.astype(jnp.float32)

    def one_expert(accum, index):
        rank_row = lax.dynamic_index_in_dim(expert_ranks, index, 0, keepdims=False)
        limit = lax.dynamic_index_in_dim(capacity, index, 0, keepdims=False)
        chosen = rank_row < limit
        chosen_int = chosen.astype(jnp.int32)
        slots = (jnp.cumsum(chosen_int).astype(jnp.int32) - chosen_int).astype(jnp.int32)
        target = jnp.where(chosen, slots, CAP).astype(jnp.int32)
        slot_rows = jnp.zeros((CAP + 1, D), jnp.float32).at[target].add(tokens_wide)[:CAP].astype(jnp.bfloat16)
        first_weight = lax.dynamic_index_in_dim(weight_in, index, 0, keepdims=False)
        second_weight = lax.dynamic_index_in_dim(weight_out, index, 0, keepdims=False)
        hidden = jnp.maximum(jnp.dot(slot_rows, first_weight, preferred_element_type=jnp.float32), 0.0).astype(jnp.bfloat16)
        expert_out = jnp.dot(hidden, second_weight, preferred_element_type=jnp.float32)
        gates = lax.dynamic_index_in_dim(gate_weights, index, 0, keepdims=False)
        scaled = (gates[:, None] * expert_out).astype(jnp.bfloat16)
        picked = jnp.take(scaled, jnp.minimum(slots, CAP - 1).astype(jnp.int32), axis=0)
        accum = accum + jnp.where(chosen[:, None], picked.astype(jnp.float32), 0.0)
        return accum, None

    accum, unused = lax.scan(one_expert, jnp.zeros((total, D), jnp.float32), jnp.arange(EXPERTS, dtype=jnp.int32))
    return accum.astype(jnp.bfloat16)
```

```python
import functools
import jax
import jax.numpy as jnp
from jax import lax
from jax.experimental import pallas as pl
from jax.experimental.pallas import tpu as pltpu
from jax.sharding import PartitionSpec as P

MOST = 8
CHUNKS = 4
PLACE_IN_F = {2: 0, 1: 1, 3: 2, 0: 3, 4: 4, 5: 5, 7: 6, 6: 7}
MESH_ID = pl.DeviceIdType.MESH
BF16 = jnp.bfloat16
F32 = jnp.float32


def ring_kernel(
    arrived, row_target, col_target, gate, w_in_hbm, w_out_hbm, out,
    w_in, w_out, own, from_left, from_right, final, hidden, part,
    back_left, back_right, stage_right, stage_left, scaled,
    w_sem, send_sem, recv_sem, back_send_sem, back_recv_sem,
):
    ring = lax.axis_size("dp")
    me = lax.axis_index("dp")
    right = lax.rem(me + 1, ring)
    left = lax.rem(me + ring - 1, ring)
    block = own.shape[2]
    cols = own.shape[3]
    half = CHUNKS // 2
    every = tuple(range(CHUNKS))
    low, high = every[:half], every[half:]
    started = []

    in_copy = pltpu.make_async_copy(w_in_hbm, w_in, w_sem.at[0])
    out_copy = pltpu.make_async_copy(w_out_hbm, w_out, w_sem.at[1])
    in_copy.start()
    out_copy.start()

    barrier = pltpu.get_barrier_semaphore()
    for other in (left, right):
        pl.semaphore_signal(barrier, inc=1, device_id={"dp": other}, device_id_type=MESH_ID)
    pl.semaphore_wait(barrier, 2)

    def copy(src, dst, sends, recvs, way, step, c):
        return pltpu.make_async_remote_copy(
            src_ref=src,
            dst_ref=dst.at[step - 1, c],
            send_sem=sends.at[way, step - 1, c],
            recv_sem=recvs.at[way, step - 1, c],
            device_id={"dp": right if way == 0 else left},
            device_id_type=MESH_ID,
        )

    def send(src, way, step, c):
        sent = copy(src, from_left if way == 0 else from_right, send_sem, recv_sem, way, step, c)
        sent.start()
        started.append(sent)

    def arrive(way, step, c):
        into = from_left if way == 0 else from_right
        copy(into.at[step - 1, c], into, send_sem, recv_sem, way, step, c).wait_recv()
        return into.at[step - 1, c]

    def send_back(src, way, step, c):
        sent = copy(
            src, back_left if way == 0 else back_right, back_send_sem, back_recv_sem, way, step, c
        )
        sent.start()
        started.append(sent)

    def arrive_back(way, step, c):
        into = back_left if way == 0 else back_right
        copy(into.at[step - 1, c], into, back_send_sem, back_recv_sem, way, step, c).wait_recv()

    def at(k, c):
        return pl.ds(PLACE_IN_F[k] * block, block), pl.ds(c * cols, cols)

    def one_hot(k):
        rows = lax.broadcasted_iota(jnp.int32, (block, arrived.shape[0]), 0) + (4 - k) * block
        return (row_target[0:1, :] == rows).astype(F32).astype(BF16)

    def place(k, c, table):
        own[k, c] = jnp.dot(
            table, arrived[:, pl.ds(c * cols, cols)], preferred_element_type=F32
        ).astype(BF16)

    first, last = one_hot(0), one_hot(4)
    for c in every:
        place(0, c, first)
        send(own.at[0, c], 0, 1, c)
        place(4, c, last)
        send(own.at[4, c], 1, 1, c)
    for k in (1, 3, 2):
        table = one_hot(k)
        for c in every:
            place(k, c, table)

    def experts(low_k, count):
        row = PLACE_IN_F[low_k] * block
        rows = count * block
        tile = min(256, w_in.shape[1])

        @pl.loop(0, w_in.shape[1] // tile)
        def _(n):
            at_n = pl.ds(pl.multiple_of(n * tile, tile), tile)
            total = jnp.dot(final[pl.ds(row, rows), :], w_in[:, at_n], preferred_element_type=F32)
            hidden[pl.ds(0, rows), at_n] = jnp.maximum(total, 0.0).astype(BF16)

        @pl.loop(0, w_out.shape[1] // tile)
        def _(n):
            at_n = pl.ds(pl.multiple_of(n * tile, tile), tile)
            part[pl.ds(row, rows), at_n] = jnp.dot(
                hidden[pl.ds(0, rows), :], w_out[:, at_n], preferred_element_type=F32
            )

    for step in range(1, 5):
        for c in every:
            ref = arrive(0, step, c)
            value = ref[...]
            total = value + own[step, c]
            ref[...] = total
            send(ref, 0, step + 1, c)
            if step == 3:
                final[at(3, c)] = value + from_right[0, c]
            if step == 4:
                final[at(4, c)] = total
            ref = arrive(1, step, c)
            value = ref[...]
            total = value + own[4 - step, c]
            ref[...] = total
            send(ref, 1, step + 1, c)
            if step == 2:
                final[at(2, c)] = value + from_left[1, c]
            if step == 3:
                final[at(1, c)] = value + from_left[0, c]
            if step == 4:
                final[at(0, c)] = total
        if step == 3:
            in_copy.wait()
            out_copy.wait()
            experts(2, 3)
        if step == 4:
            experts(0, 2)
    for c in every:
        ref = arrive(0, 5, c)
        if c in low:
            send(ref, 0, 6, c)
        final[at(5, c)] = ref[...]
        ref = arrive(1, 5, c)
        if c in high:
            send(ref, 1, 6, c)
        final[at(7, c)] = ref[...]
    experts(5, 2)
    for c in high:
        stage_right[1, c] = part[at(7, c)].astype(BF16)
        send_back(stage_right.at[1, c], 0, 2, c)
    for c in low:
        stage_left[1, c] = part[at(5, c)].astype(BF16)
        send_back(stage_left.at[1, c], 1, 2, c)
    for c in low:
        final[at(6, c)] = arrive(0, 6, c)[...]
    for c in high:
        final[at(6, c)] = arrive(1, 6, c)[...]
    experts(6, 1)
    for c in low:
        stage_right[0, c] = part[at(6, c)].astype(BF16)
        send_back(stage_right.at[0, c], 0, 1, c)
    for c in high:
        stage_left[0, c] = part[at(6, c)].astype(BF16)
        send_back(stage_left.at[0, c], 1, 1, c)
    for c in low:
        arrive_back(0, 1, c)
        stage_right[1, c] = (part[at(7, c)] + back_left[0, c].astype(F32)).astype(BF16)
        send_back(stage_right.at[1, c], 0, 2, c)
    for c in high:
        arrive_back(1, 1, c)
        stage_left[1, c] = (part[at(5, c)] + back_right[0, c].astype(F32)).astype(BF16)
        send_back(stage_left.at[1, c], 1, 2, c)

    def finish(k, c, total):
        rows = pl.ds((4 - k) * block, block)
        scaled[rows, pl.ds(c * cols, cols)] = (gate[rows, 0:1] * total).astype(BF16)

    for step in range(2, 7):
        for c in every:
            k = step - 2
            arrive_back(0, step, c)
            total = part[at(k, c)] + back_left[step - 1, c].astype(F32)
            if step < 6:
                stage_right[step, c] = total.astype(BF16)
                send_back(stage_right.at[step, c], 0, step + 1, c)
            if step == 5:
                finish(3, c, total + back_right[2, c].astype(F32))
            if step == 6:
                finish(4, c, total + back_right[1, c].astype(F32))
            k = 6 - step
            arrive_back(1, step, c)
            total = part[at(k, c)] + back_right[step - 1, c].astype(F32)
            if step < 6:
                stage_left[step, c] = total.astype(BF16)
                send_back(stage_left.at[step, c], 1, step + 1, c)
            if step == 4:
                finish(2, c, total + back_left[3, c].astype(F32))
            if step == 5:
                finish(1, c, total + back_left[2, c].astype(F32))
            if step == 6:
                finish(0, c, total + back_left[1, c].astype(F32))
    window = 5 * block
    table = (
        col_target[:, 0:1] == lax.broadcasted_iota(jnp.int32, (arrived.shape[0], window), 1)
    ).astype(F32).astype(BF16)
    for c in every:
        at_c = pl.ds(c * cols, cols)
        out[:, at_c] = jnp.dot(table, scaled[:, at_c], preferred_element_type=F32).astype(BF16)
    for sent in started:
        sent.wait_send()


def ring_stage(arrived, row_target, col_target, gate, w_in, w_out):
    rows, width = arrived.shape
    block = rows // 2
    cols = width // CHUNKS
    units = w_in.shape[1]
    slots = (6, CHUNKS, block, cols)
    vmem = pl.BlockSpec(memory_space=pltpu.VMEM)
    anywhere = pl.BlockSpec(memory_space=pl.ANY)
    sems = pltpu.SemaphoreType.DMA((2, 6, CHUNKS))
    return pl.pallas_call(
        ring_kernel,
        out_shape=jax.ShapeDtypeStruct((rows, width), BF16),
        in_specs=[vmem] * 4 + [anywhere] * 2,
        out_specs=vmem,
        scratch_shapes=[
            pltpu.VMEM(w_in.shape, BF16),
            pltpu.VMEM(w_out.shape, BF16),
            pltpu.VMEM((5, CHUNKS, block, cols), BF16),
            pltpu.VMEM(slots, BF16),
            pltpu.VMEM(slots, BF16),
            pltpu.VMEM((8 * block, width), BF16),
            pltpu.VMEM((3 * block, units), BF16),
            pltpu.VMEM((8 * block, width), F32),
            pltpu.VMEM(slots, BF16),
            pltpu.VMEM(slots, BF16),
            pltpu.VMEM(slots, BF16),
            pltpu.VMEM(slots, BF16),
            pltpu.VMEM((5 * block, width), BF16),
            pltpu.SemaphoreType.DMA((2,)),
            sems, sems, sems, sems,
        ],
        compiler_params=pltpu.CompilerParams(
            collective_id=0, has_side_effects=True, vmem_limit_bytes=62 * 1024 * 1024
        ),
        name="ring",
    )(arrived, row_target, col_target, gate, w_in, w_out)


def placement(arrived_counts, plane_counts, me, block):
    planes = plane_counts.shape[0]
    index = lax.broadcasted_iota(jnp.int32, (planes,), 0)
    spare = 2 * block - plane_counts
    left_over = planes * block - jnp.sum(plane_counts)
    padded = plane_counts + jnp.clip(left_over - (jnp.cumsum(spare) - spare), 0, spare)
    drift = jnp.cumsum(padded) - padded - block * index
    mine = index == me
    base = jnp.sum(jnp.where(mine, drift, 0)) - jnp.max(drift) + 4 * block
    first_slot = jnp.sum(jnp.where(index < me, plane_counts, 0))
    starts = jnp.cumsum(arrived_counts) - arrived_counts
    within = lax.broadcasted_iota(jnp.int32, (arrived_counts.shape[0], MOST), 1)
    target = jnp.where(within < arrived_counts[:, None], base + starts[:, None] + within, -1)
    return target.reshape(-1), base, first_slot


def on_device(tokens, expert_ranks, capacity, weight_in, weight_out, gate_weights):
    planes = lax.axis_size("dp")
    expert_count = lax.axis_size("expert")
    me = lax.axis_index("dp")
    token_count, width = tokens.shape
    block = gate_weights.shape[1]
    slots_all = block * planes
    chosen = expert_ranks < capacity[:, None]
    chosen_int = chosen.astype(jnp.int32)
    counts = jnp.sum(chosen_int, axis=1)
    before = jnp.cumsum(chosen_int, axis=1) - chosen_int
    places = lax.broadcasted_iota(jnp.int32, (expert_count, MOST, token_count), 1)
    pack_table = jnp.logical_and(chosen[:, None, :], before[:, None, :] == places)
    pack_table = pack_table.astype(BF16).reshape(expert_count * MOST, token_count)
    packed = jnp.dot(pack_table, tokens, preferred_element_type=F32).astype(BF16)
    arrived_counts = lax.all_to_all(
        counts.reshape(expert_count, 1), "expert", split_axis=0, concat_axis=0, tiled=True
    ).reshape(expert_count)
    plane_counts = lax.all_gather(jnp.sum(arrived_counts), "dp")
    gates = lax.all_gather(gate_weights[0], "dp").reshape(slots_all)
    arrived = lax.all_to_all(
        packed.reshape(expert_count, MOST, width), "expert", split_axis=0, concat_axis=0, tiled=True
    ).reshape(expert_count * MOST, width)
    target, base, first_slot = placement(arrived_counts, plane_counts, me, block)
    slot = first_slot - base + lax.broadcasted_iota(jnp.int32, (5 * block, slots_all), 0)
    slot_ids = lax.broadcasted_iota(jnp.int32, (5 * block, slots_all), 1)
    window_gate = jnp.sum(jnp.where(slot == slot_ids, gates[None, :], 0.0), axis=1)
    returned = ring_stage(
        arrived,
        jnp.broadcast_to(target[None, :], (8, target.shape[0])),
        jnp.broadcast_to(target[:, None], (target.shape[0], 128)),
        jnp.broadcast_to(window_gate[:, None], (5 * block, 128)),
        weight_in[0],
        weight_out[0],
    )
    results = lax.all_to_all(
        returned.reshape(expert_count, MOST, width), "expert", split_axis=0, concat_axis=0, tiled=True
    )
    combined = lax.dot_general(
        pack_table,
        results.reshape(expert_count * MOST, width),
        (((0,), (0,)), ((), ())),
        preferred_element_type=F32,
    )
    return combined.astype(BF16)


def solution(mesh):
    both = ("dp", "expert")
    placed = (
        P(both, None),
        P(None, both),
        P(),
        P("expert", None, "dp"),
        P("expert", "dp", None),
        P("expert", "dp"),
    )
    return jax.shard_map(
        on_device, mesh=mesh, in_specs=placed, out_specs=P(both, None), check_vma=False
    )
```

```python
import jax
import jax.numpy as jnp
from jax import lax
from jax.experimental import pallas as pl
from jax.experimental.pallas import tpu as pltpu
from jax.sharding import PartitionSpec as P

MOST = 8
CHUNKS = 4
LANES = 128
PLACE_IN_F = {2: 0, 1: 1, 3: 2, 0: 3, 4: 4, 5: 5, 7: 6, 6: 7}
MESH_ID = pl.DeviceIdType.MESH
BF16 = jnp.bfloat16
F32 = jnp.float32


def iota(shape, dim):
    return lax.broadcasted_iota(jnp.int32, shape, dim)


def dot(a, b):
    return jnp.dot(a, b, preferred_element_type=F32)


def table_of(mask):
    return jnp.where(mask, 1.0, 0.0).astype(BF16)


def layer_kernel(
    capacity, tokens, ranks, gate_in, w_in_hbm, w_out_hbm, out,
    w_in, w_out, own, from_left, from_right, final, hidden, part,
    back_left, back_right, stage_right, stage_left, scaled,
    packed, arrived, returned, results, counts_out, counts_in, totals_out, totals_in,
    gates_out, gates_in, window_gate, place_table, target_column, take_table,
    w_sem, send_sem, recv_sem, back_send_sem, back_recv_sem,
    rows_send, rows_recv, out_send, out_recv, small_send, small_recv,
):
    planes = lax.axis_size("dp")
    experts_all = lax.axis_size("expert")
    me = lax.axis_index("dp")
    my_expert = lax.axis_index("expert")
    right = lax.rem(me + 1, planes)
    left = lax.rem(me + planes - 1, planes)
    block = own.shape[2]
    cols = own.shape[3]
    rows_all = experts_all * MOST
    window = 5 * block
    half = CHUNKS // 2
    every = tuple(range(CHUNKS))
    low, high = every[:half], every[half:]
    started = []

    barrier = pltpu.get_barrier_semaphore()

    @pl.loop(1, experts_all)
    def _(i):
        peer = lax.rem(my_expert + i, experts_all)
        pl.semaphore_signal(barrier, inc=1, device_id={"expert": peer}, device_id_type=MESH_ID)

    @pl.loop(1, planes)
    def _(i):
        peer = lax.rem(me + i, planes)
        pl.semaphore_signal(barrier, inc=1, device_id={"dp": peer}, device_id_type=MESH_ID)

    in_copy = pltpu.make_async_copy(w_in_hbm, w_in, w_sem.at[0])
    out_copy = pltpu.make_async_copy(w_out_hbm, w_out, w_sem.at[1])
    in_copy.start()
    out_copy.start()

    def columns(c):
        return pl.ds(c * cols, cols)

    def grouped(value):
        return value.reshape(experts_all, MOST, value.shape[-1])

    def flat(value):
        return value.astype(F32).reshape(rows_all, value.shape[-1])

    def to_all_experts(src_of, dst, sends, recvs):
        @pl.loop(1, experts_all)
        def _(i):
            peer = lax.rem(my_expert + i, experts_all)
            pltpu.make_async_remote_copy(
                src_ref=src_of(peer),
                dst_ref=dst.at[my_expert],
                send_sem=sends,
                recv_sem=recvs,
                device_id={"expert": peer},
                device_id_type=MESH_ID,
            ).start()

    def to_all_planes(src, dst, sends, recvs):
        @pl.loop(1, planes)
        def _(i):
            peer = lax.rem(me + i, planes)
            pltpu.make_async_remote_copy(
                src_ref=src,
                dst_ref=dst.at[me],
                send_sem=sends,
                recv_sem=recvs,
                device_id={"dp": peer},
                device_id_type=MESH_ID,
            ).start()

    def wait_all(ref, count, sem):
        several = ref.at[pl.ds(0, count)]
        pltpu.make_async_copy(several, several, sem).wait()

    limits = jnp.zeros((experts_all, LANES), jnp.int32)
    for e in range(experts_all):
        limits = jnp.where(iota((experts_all, LANES), 0) == e, capacity[e], limits)
    token_count = tokens.shape[0]
    chosen = ranks[...] < limits[:, 0:1]
    chosen_table = table_of(chosen)
    earlier = table_of(iota((token_count, token_count), 0) < iota((token_count, token_count), 1))
    code = jnp.where(chosen, dot(chosen_table, earlier), -1.0).astype(BF16)
    expand = table_of(
        iota((rows_all, experts_all), 0) // MOST == iota((rows_all, experts_all), 1)
    )
    row_counts = dot(
        expand, dot(chosen_table, jnp.ones((token_count, LANES), BF16)).astype(BF16)
    )
    counts_out[...] = grouped(row_counts)
    gates_out[...] = jnp.broadcast_to(gate_in[...], gates_out.shape)
    within = (iota((rows_all, token_count), 0) % MOST).astype(F32)
    pack = jnp.where(dot(expand, code) == within, 1.0, 0.0)
    pack_table = pack.astype(BF16)
    for c in every:
        packed[c] = grouped(dot(pack_table, tokens[:, columns(c)])).astype(BF16)
        arrived[c, my_expert] = packed[c, my_expert]
    counts_in[my_expert] = counts_out[my_expert]
    gates_in[me] = gates_out[...]

    pl.semaphore_wait(barrier, experts_all + planes - 2)
    to_all_experts(lambda peer: counts_out.at[peer], counts_in, small_send.at[0], small_recv.at[0])
    to_all_experts(lambda peer: packed.at[0, peer], arrived.at[0], rows_send.at[0], rows_recv.at[0])

    wait_all(counts_in, experts_all - 1, small_recv.at[0])
    counts = counts_in[...].reshape(rows_all, LANES)
    counts_table = counts.astype(BF16)
    lead = iota((MOST, rows_all), 1) % MOST == 0
    totals_out[...] = dot(table_of(lead), counts_table)
    totals_in[me] = totals_out[...]
    to_all_planes(totals_out, totals_in, small_send.at[1], small_recv.at[1])
    to_all_planes(gates_out, gates_in, small_send.at[2], small_recv.at[2])
    for c in every[1:]:
        to_all_experts(
            lambda peer: packed.at[c, peer], arrived.at[c], rows_send.at[c], rows_recv.at[c]
        )
    row_ids = iota((rows_all, rows_all), 0)
    lane_ids = iota((rows_all, rows_all), 1)
    ahead = jnp.logical_and(lane_ids % MOST == 0, lane_ids // MOST < row_ids // MOST)
    starts = dot(table_of(ahead), counts_table)
    place_in = (iota((rows_all, LANES), 0) % MOST).astype(F32)
    take_table[...] = pack.T.astype(BF16)
    wait_all(totals_in, planes - 1, small_recv.at[1])
    plane_counts = [totals_in[z] for z in range(planes)]
    left_over = jnp.full((MOST, LANES), float(planes * block), F32)
    for z in range(planes):
        left_over = left_over - plane_counts[z]
    padded_start = jnp.zeros((MOST, LANES), F32)
    first_slot = padded_start
    drift_mine = padded_start
    drift_most = padded_start
    for z in range(planes):
        drift = padded_start - float(z * block)
        drift_most = jnp.maximum(drift_most, drift)
        drift_mine = jnp.where(me == z, drift, drift_mine)
        first_slot = first_slot + jnp.where(me > z, plane_counts[z], 0.0)
        extra = jnp.minimum(2.0 * block - plane_counts[z], left_over)
        left_over = left_over - extra
        padded_start = padded_start + plane_counts[z] + extra
    base = drift_mine - drift_most + 4.0 * block
    target = jnp.where(place_in < counts, base[0:1, :] + starts + place_in, -1.0)
    target_column[...] = target
    target_row = target.T[0:1, :]
    place_table[...] = table_of(target_row == iota((window, rows_all), 0).astype(F32))

    def copy(src, dst, sends, recvs, way, step, c):
        return pltpu.make_async_remote_copy(
            src_ref=src,
            dst_ref=dst.at[step - 1, c],
            send_sem=sends.at[way, step - 1, c],
            recv_sem=recvs.at[way, step - 1, c],
            device_id={"dp": right if way == 0 else left},
            device_id_type=MESH_ID,
        )

    def send(src, way, step, c):
        sent = copy(src, from_left if way == 0 else from_right, send_sem, recv_sem, way, step, c)
        sent.start()
        started.append(sent)

    def arrive(way, step, c):
        into = from_left if way == 0 else from_right
        copy(into.at[step - 1, c], into, send_sem, recv_sem, way, step, c).wait_recv()
        return into.at[step - 1, c]

    def send_back(src, way, step, c):
        sent = copy(
            src, back_left if way == 0 else back_right, back_send_sem, back_recv_sem, way, step, c
        )
        sent.start()
        started.append(sent)

    def arrive_back(way, step, c):
        into = back_left if way == 0 else back_right
        copy(into.at[step - 1, c], into, back_send_sem, back_recv_sem, way, step, c).wait_recv()

    def at(k, c):
        return pl.ds(PLACE_IN_F[k] * block, block), columns(c)

    def place(k, c, rows):
        own[k, c] = dot(place_table[pl.ds((4 - k) * block, block), :], rows).astype(BF16)

    def arrived_rows(c):
        return flat(arrived[c]).astype(BF16)

    for c in every:
        wait_all(arrived.at[c], experts_all - 1, rows_recv.at[c])
        rows = arrived_rows(c)
        place(0, c, rows)
        send(own.at[0, c], 0, 1, c)
        place(4, c, rows)
        send(own.at[4, c], 1, 1, c)
        for k in (1, 3, 2):
            place(k, c, rows)

    def experts(low_k, count):
        row = PLACE_IN_F[low_k] * block
        rows = count * block
        tile = min(256, w_in.shape[1])

        @pl.loop(0, w_in.shape[1] // tile)
        def _(n):
            at_n = pl.ds(pl.multiple_of(n * tile, tile), tile)
            total = dot(final[pl.ds(row, rows), :], w_in[:, at_n])
            hidden[pl.ds(0, rows), at_n] = jnp.maximum(total, 0.0).astype(BF16)

        @pl.loop(0, w_out.shape[1] // tile)
        def _(n):
            at_n = pl.ds(pl.multiple_of(n * tile, tile), tile)
            part[pl.ds(row, rows), at_n] = dot(hidden[pl.ds(0, rows), :], w_out[:, at_n])

    for step in range(1, 5):
        for c in every:
            ref = arrive(0, step, c)
            value = ref[...]
            total = value + own[step, c]
            ref[...] = total
            send(ref, 0, step + 1, c)
            if step == 3:
                final[at(3, c)] = value + from_right[0, c]
            if step == 4:
                final[at(4, c)] = total
            ref = arrive(1, step, c)
            value = ref[...]
            total = value + own[4 - step, c]
            ref[...] = total
            send(ref, 1, step + 1, c)
            if step == 2:
                final[at(2, c)] = value + from_left[1, c]
            if step == 3:
                final[at(1, c)] = value + from_left[0, c]
            if step == 4:
                final[at(0, c)] = total
        if step == 1:
            wait_all(gates_in, planes - 1, small_recv.at[2])
            shift = (first_slot - base)[0:1, 0:1]
            gap = (iota((window, block), 1) - iota((window, block), 0)).astype(F32)
            total = jnp.zeros((window, block), F32)
            for z in range(planes):
                total = total + jnp.where(gap + float(z * block) == shift, gates_in[z][0:1, :], 0.0)
            window_gate[...] = jnp.broadcast_to(
                jnp.sum(total, axis=1, keepdims=True), window_gate.shape
            )
        if step == 3:
            in_copy.wait()
            out_copy.wait()
            experts(2, 3)
        if step == 4:
            experts(0, 2)
    for c in every:
        ref = arrive(0, 5, c)
        if c in low:
            send(ref, 0, 6, c)
        final[at(5, c)] = ref[...]
        ref = arrive(1, 5, c)
        if c in high:
            send(ref, 1, 6, c)
        final[at(7, c)] = ref[...]
    experts(5, 2)
    for c in high:
        stage_right[1, c] = part[at(7, c)].astype(BF16)
        send_back(stage_right.at[1, c], 0, 2, c)
    for c in low:
        stage_left[1, c] = part[at(5, c)].astype(BF16)
        send_back(stage_left.at[1, c], 1, 2, c)
    for c in low:
        final[at(6, c)] = arrive(0, 6, c)[...]
    for c in high:
        final[at(6, c)] = arrive(1, 6, c)[...]
    experts(6, 1)
    for c in low:
        stage_right[0, c] = part[at(6, c)].astype(BF16)
        send_back(stage_right.at[0, c], 0, 1, c)
    for c in high:
        stage_left[0, c] = part[at(6, c)].astype(BF16)
        send_back(stage_left.at[0, c], 1, 1, c)
    for c in low:
        arrive_back(0, 1, c)
        stage_right[1, c] = (part[at(7, c)] + back_left[0, c].astype(F32)).astype(BF16)
        send_back(stage_right.at[1, c], 0, 2, c)
    for c in high:
        arrive_back(1, 1, c)
        stage_left[1, c] = (part[at(5, c)] + back_right[0, c].astype(F32)).astype(BF16)
        send_back(stage_left.at[1, c], 1, 2, c)

    def finish(k, c, total):
        rows = pl.ds((4 - k) * block, block)
        scaled[rows, columns(c)] = (window_gate[rows, 0:1] * total).astype(BF16)

    pick_table = table_of(
        target_column[:, 0:1] == iota((rows_all, window), 1).astype(F32)
    )
    for step in range(2, 7):
        for c in every:
            k = step - 2
            arrive_back(0, step, c)
            total = part[at(k, c)] + back_left[step - 1, c].astype(F32)
            if step < 6:
                stage_right[step, c] = total.astype(BF16)
                send_back(stage_right.at[step, c], 0, step + 1, c)
            if step == 5:
                finish(3, c, total + back_right[2, c].astype(F32))
            if step == 6:
                finish(4, c, total + back_right[1, c].astype(F32))
            k = 6 - step
            arrive_back(1, step, c)
            total = part[at(k, c)] + back_right[step - 1, c].astype(F32)
            if step < 6:
                stage_left[step, c] = total.astype(BF16)
                send_back(stage_left.at[step, c], 1, step + 1, c)
            if step == 4:
                finish(2, c, total + back_left[3, c].astype(F32))
            if step == 5:
                finish(1, c, total + back_left[2, c].astype(F32))
            if step == 6:
                finish(0, c, total + back_left[1, c].astype(F32))
                returned[c] = grouped(dot(pick_table, scaled[:, columns(c)])).astype(BF16)
                to_all_experts(
                    lambda peer: returned.at[c, peer], results.at[c], out_send.at[c], out_recv.at[c]
                )
                results[c, my_expert] = returned[c, my_expert]
    for c in every:
        wait_all(results.at[c], experts_all - 1, out_recv.at[c])
        out[:, columns(c)] = dot(take_table[...], flat(results[c]).astype(BF16)).astype(BF16)

    for sent in started:
        sent.wait_send()
    wait_all(counts_out, experts_all - 1, small_send.at[0])
    wait_all(totals_in, planes - 1, small_send.at[1])
    wait_all(gates_in, planes - 1, small_send.at[2])
    for c in every:
        wait_all(packed.at[c], experts_all - 1, rows_send.at[c])
        wait_all(returned.at[c], experts_all - 1, out_send.at[c])


def on_device(tokens, expert_ranks, capacity, weight_in, weight_out, gate_weights):
    planes = lax.axis_size("dp")
    experts_all = lax.axis_size("expert")
    token_count, width = tokens.shape
    block = gate_weights.shape[1]
    units = weight_in.shape[2]
    cols = width // CHUNKS
    rows_all = experts_all * MOST
    vmem = pl.BlockSpec(memory_space=pltpu.VMEM)
    anywhere = pl.BlockSpec(memory_space=pl.ANY)
    slots = pltpu.VMEM((6, CHUNKS, block, cols), BF16)
    exchange = pltpu.VMEM((CHUNKS, experts_all, MOST, cols), BF16)
    ring_sems = pltpu.SemaphoreType.DMA((2, 6, CHUNKS))
    chunk_sems = pltpu.SemaphoreType.DMA((CHUNKS,))
    return pl.pallas_call(
        layer_kernel,
        out_shape=jax.ShapeDtypeStruct((token_count, width), BF16),
        in_specs=[pl.BlockSpec(memory_space=pltpu.SMEM)] + [vmem] * 3 + [anywhere] * 2,
        out_specs=vmem,
        scratch_shapes=[
            pltpu.VMEM(weight_in.shape[1:], BF16),
            pltpu.VMEM(weight_out.shape[1:], BF16),
            pltpu.VMEM((5, CHUNKS, block, cols), BF16),
            slots, slots,
            pltpu.VMEM((8 * block, width), BF16),
            pltpu.VMEM((3 * block, units), BF16),
            pltpu.VMEM((8 * block, width), F32),
            slots, slots, slots, slots,
            pltpu.VMEM((5 * block, width), BF16),
            exchange, exchange, exchange, exchange,
            pltpu.VMEM((experts_all, MOST, LANES), F32),
            pltpu.VMEM((experts_all, MOST, LANES), F32),
            pltpu.VMEM((MOST, LANES), F32),
            pltpu.VMEM((planes, MOST, LANES), F32),
            pltpu.VMEM((MOST, block), F32),
            pltpu.VMEM((planes, MOST, block), F32),
            pltpu.VMEM((5 * block, LANES), F32),
            pltpu.VMEM((5 * block, rows_all), BF16),
            pltpu.VMEM((rows_all, LANES), F32),
            pltpu.VMEM((token_count, rows_all), BF16),
            pltpu.SemaphoreType.DMA((2,)),
            ring_sems, ring_sems, ring_sems, ring_sems,
            chunk_sems, chunk_sems, chunk_sems, chunk_sems,
            pltpu.SemaphoreType.DMA((3,)),
            pltpu.SemaphoreType.DMA((3,)),
        ],
        compiler_params=pltpu.CompilerParams(
            collective_id=0, has_side_effects=True, vmem_limit_bytes=63 * 1024 * 1024
        ),
        name="layer",
    )(capacity, tokens, expert_ranks, gate_weights, weight_in[0], weight_out[0])


def solution(mesh):
    both = ("dp", "expert")
    placed = (
        P(both, None),
        P(None, both),
        P(),
        P("expert", None, "dp"),
        P("expert", "dp", None),
        P("expert", "dp"),
    )
    return jax.shard_map(
        on_device, mesh=mesh, in_specs=placed, out_specs=P(both, None), check_vma=False
    )
```

```python
import jax
import jax.numpy as jnp
from jax import lax
from jax.experimental import pallas as pl
from jax.experimental.pallas import tpu as pltpu
from jax.sharding import PartitionSpec as P

MOST = 8
SIXTEENTHS = (4, 4, 4, 2, 2)
FIRST_HALF = 2
LANES = 128
PLACE_IN_F = {2: 0, 1: 1, 3: 2, 0: 3, 4: 4, 5: 5, 7: 6, 6: 7}
MESH_ID = pl.DeviceIdType.MESH
BF16 = jnp.bfloat16
F32 = jnp.float32


def iota(shape, dim):
    return lax.broadcasted_iota(jnp.int32, shape, dim)


def dot(a, b):
    return jnp.dot(a, b, preferred_element_type=F32)


def table_of(mask):
    return jnp.where(mask, 1.0, 0.0).astype(BF16)


def layer_kernel(
    capacity, tokens_hbm, ranks_hbm, gate_hbm, w_in_hbm, w_out_hbm, out,
    tokens, ranks, gate_in, w_in, w_out, own, from_left, from_right, final, hidden, part,
    back_left, back_right, stage_right, stage_left, scaled,
    packed, arrived, returned, results, counts_out, counts_in, counts_flat, totals_out, totals_in,
    gates_out, gates_in, window_gate, place_table, target_column, take_table,
    in_sem, send_sem, recv_sem, back_send_sem, back_recv_sem,
    rows_send, rows_recv, out_send, out_recv, small_send, small_recv,
):
    planes = lax.axis_size("dp")
    experts_all = lax.axis_size("expert")
    me = lax.axis_index("dp")
    my_expert = lax.axis_index("expert")
    right = lax.rem(me + 1, planes)
    left = lax.rem(me + planes - 1, planes)
    block = own.shape[1]
    width = own.shape[2]
    widths = [width // 16 * share for share in SIXTEENTHS]
    rows_all = experts_all * MOST
    window = 5 * block
    every = tuple(range(len(widths)))
    half = FIRST_HALF
    low, high = every[:half], every[half:]
    started = []

    loads = [
        pltpu.make_async_copy(src, dst, in_sem.at[n])
        for n, (src, dst) in enumerate(
            (
                (ranks_hbm, ranks),
                (gate_hbm, gate_in),
                (tokens_hbm, tokens),
                (w_in_hbm, w_in),
                (w_out_hbm, w_out),
            )
        )
    ]
    for load in loads[:3]:
        load.start()

    def partner(i):
        return lax.rem(my_expert + i + 1, experts_all)

    barrier = pltpu.get_barrier_semaphore()

    @pl.loop(0, experts_all - 1)
    def _(i):
        peer = partner(i)
        pl.semaphore_signal(barrier, inc=1, device_id={"expert": peer}, device_id_type=MESH_ID)

    @pl.loop(1, planes)
    def _(i):
        peer = lax.rem(me + i, planes)
        pl.semaphore_signal(barrier, inc=1, device_id={"dp": peer}, device_id_type=MESH_ID)

    def columns(c):
        return pl.ds(sum(widths[:c]), widths[c])

    def grouped(value):
        return value.reshape(experts_all, MOST, value.shape[-1])

    def flat(value):
        return value.astype(F32).reshape(rows_all, value.shape[-1])

    def to_all_experts(src_of, dst, sends, recvs):
        @pl.loop(0, experts_all - 1, unroll=True)
        def _(i):
            peer = partner(i)
            pltpu.make_async_remote_copy(
                src_ref=src_of(peer),
                dst_ref=dst.at[my_expert],
                send_sem=sends,
                recv_sem=recvs,
                device_id={"expert": peer},
                device_id_type=MESH_ID,
            ).start()

    def to_all_planes(src, dst, sends, recvs):
        @pl.loop(1, planes)
        def _(i):
            peer = lax.rem(me + i, planes)
            pltpu.make_async_remote_copy(
                src_ref=src,
                dst_ref=dst.at[me],
                send_sem=sends,
                recv_sem=recvs,
                device_id={"dp": peer},
                device_id_type=MESH_ID,
            ).start()

    def wait_all(ref, count, sem):
        several = ref.at[pl.ds(0, count)]
        pltpu.make_async_copy(several, several, sem).wait()

    def rows_of(ref, c):
        return ref.at[:, :, columns(c)]

    limits = jnp.zeros((experts_all, LANES), jnp.int32)
    for e in range(experts_all):
        limits = jnp.where(iota((experts_all, LANES), 0) == e, capacity[e], limits)
    token_count = tokens.shape[0]
    loads[0].wait()
    chosen = ranks[...] < limits[:, 0:1]
    chosen_table = table_of(chosen)
    taken = dot(chosen_table, jnp.ones((token_count, LANES), BF16))
    for e in range(experts_all):
        counts_out[e] = taken[e : e + 1, :]
    counts_in[my_expert] = counts_out[my_expert]
    loads[1].wait()
    gates_out[...] = jnp.broadcast_to(gate_in[...], gates_out.shape)
    gates_in[me] = gates_out[...]

    pl.semaphore_wait(barrier, experts_all + planes - 2)
    to_all_experts(lambda peer: counts_out.at[peer], counts_in, small_send.at[0], small_recv.at[0])
    to_all_planes(gates_out, gates_in, small_send.at[2], small_recv.at[2])

    earlier = table_of(iota((token_count, token_count), 0) < iota((token_count, token_count), 1))
    code = jnp.where(chosen, dot(chosen_table, earlier), -1.0).astype(BF16)
    expand = table_of(
        iota((rows_all, experts_all), 0) // MOST == iota((rows_all, experts_all), 1)
    )
    within = (iota((rows_all, token_count), 0) % MOST).astype(F32)
    pack = jnp.where(dot(expand, code) == within, 1.0, 0.0)
    pack_table = pack.astype(BF16)

    def pack_rows(c):
        packed[:, :, columns(c)] = grouped(dot(pack_table, tokens[:, columns(c)])).astype(BF16)
        to_all_experts(
            lambda peer: rows_of(packed, c).at[peer],
            rows_of(arrived, c),
            rows_send.at[c],
            rows_recv.at[c],
        )
        arrived[my_expert, :, columns(c)] = packed[my_expert, :, columns(c)]

    loads[2].wait()
    for load in loads[3:]:
        load.start()
    pack_rows(0)
    pack_rows(1)

    wait_all(counts_in, experts_all - 1, small_recv.at[0])
    for e in range(experts_all):
        counts_flat[e : e + 1, :] = counts_in[e]
    counts = dot(expand, counts_flat[...].astype(BF16))
    totals_out[...] = jnp.broadcast_to(
        jnp.sum(counts_flat[...], axis=0, keepdims=True), totals_out.shape
    )
    to_all_planes(totals_out, totals_in, small_send.at[1], small_recv.at[1])
    totals_in[me] = totals_out[...]
    for c in every[2:]:
        pack_rows(c)
    counts_table = counts.astype(BF16)
    row_ids = iota((rows_all, rows_all), 0)
    lane_ids = iota((rows_all, rows_all), 1)
    ahead = jnp.logical_and(lane_ids % MOST == 0, lane_ids // MOST < row_ids // MOST)
    starts = dot(table_of(ahead), counts_table)
    place_in = (iota((rows_all, LANES), 0) % MOST).astype(F32)
    take_table[...] = pack.T.astype(BF16)
    wait_all(totals_in, planes - 1, small_recv.at[1])
    plane_counts = [totals_in[z] for z in range(planes)]
    left_over = jnp.full((MOST, LANES), float(planes * block), F32)
    for z in range(planes):
        left_over = left_over - plane_counts[z]
    padded_start = jnp.zeros((MOST, LANES), F32)
    first_slot = padded_start
    drift_mine = padded_start
    drift_most = padded_start
    for z in range(planes):
        drift = padded_start - float(z * block)
        drift_most = jnp.maximum(drift_most, drift)
        drift_mine = jnp.where(me == z, drift, drift_mine)
        first_slot = first_slot + jnp.where(me > z, plane_counts[z], 0.0)
        extra = jnp.minimum(2.0 * block - plane_counts[z], left_over)
        left_over = left_over - extra
        padded_start = padded_start + plane_counts[z] + extra
    base = drift_mine - drift_most + 4.0 * block
    target = jnp.where(place_in < counts, base[0:1, :] + starts + place_in, -1.0)
    target_column[...] = target
    target_row = target.T[0:1, :]
    place_table[...] = table_of(target_row == iota((window, rows_all), 0).astype(F32))

    def copy(src, dst, sends, recvs, way, step, c):
        return pltpu.make_async_remote_copy(
            src_ref=src,
            dst_ref=dst.at[step - 1, :, columns(c)],
            send_sem=sends.at[way, step - 1, c],
            recv_sem=recvs.at[way, step - 1, c],
            device_id={"dp": right if way == 0 else left},
            device_id_type=MESH_ID,
        )

    def send(src, way, step, c):
        sent = copy(src, from_left if way == 0 else from_right, send_sem, recv_sem, way, step, c)
        sent.start()
        started.append(sent)

    def arrive(way, step, c):
        into = from_left if way == 0 else from_right
        ref = into.at[step - 1, :, columns(c)]
        copy(ref, into, send_sem, recv_sem, way, step, c).wait_recv()
        return ref

    def send_back(src, way, step, c):
        sent = copy(
            src, back_left if way == 0 else back_right, back_send_sem, back_recv_sem, way, step, c
        )
        sent.start()
        started.append(sent)

    def arrive_back(way, step, c):
        into = back_left if way == 0 else back_right
        ref = into.at[step - 1, :, columns(c)]
        copy(ref, into, back_send_sem, back_recv_sem, way, step, c).wait_recv()

    def at(k, c):
        return pl.ds(PLACE_IN_F[k] * block, block), columns(c)

    def place(k, c, rows):
        own[k, :, columns(c)] = dot(place_table[pl.ds((4 - k) * block, block), :], rows).astype(BF16)

    def arrived_rows(c):
        return flat(arrived[:, :, columns(c)]).astype(BF16)

    for c in every:
        wait_all(rows_of(arrived, c), experts_all - 1, rows_recv.at[c])
        rows = arrived_rows(c)
        place(0, c, rows)
        send(own.at[0, :, columns(c)], 0, 1, c)
        place(4, c, rows)
        send(own.at[4, :, columns(c)], 1, 1, c)
        for k in (1, 3, 2):
            place(k, c, rows)

    def experts(low_k, count):
        row = PLACE_IN_F[low_k] * block
        rows = count * block
        tile = min(256, w_in.shape[1])

        @pl.loop(0, w_in.shape[1] // tile)
        def _(n):
            at_n = pl.ds(pl.multiple_of(n * tile, tile), tile)
            total = dot(final[pl.ds(row, rows), :], w_in[:, at_n])
            hidden[pl.ds(0, rows), at_n] = jnp.maximum(total, 0.0).astype(BF16)

        @pl.loop(0, w_out.shape[1] // tile)
        def _(n):
            at_n = pl.ds(pl.multiple_of(n * tile, tile), tile)
            part[pl.ds(row, rows), at_n] = dot(hidden[pl.ds(0, rows), :], w_out[:, at_n])

    for step in range(1, 5):
        for c in every:
            ref = arrive(0, step, c)
            value = ref[...]
            total = value + own[step, :, columns(c)]
            ref[...] = total
            send(ref, 0, step + 1, c)
            if step == 3:
                final[at(3, c)] = value + from_right[0, :, columns(c)]
            if step == 4:
                final[at(4, c)] = total
            ref = arrive(1, step, c)
            value = ref[...]
            total = value + own[4 - step, :, columns(c)]
            ref[...] = total
            send(ref, 1, step + 1, c)
            if step == 2:
                final[at(2, c)] = value + from_left[1, :, columns(c)]
            if step == 3:
                final[at(1, c)] = value + from_left[0, :, columns(c)]
            if step == 4:
                final[at(0, c)] = total
        if step == 1:
            wait_all(gates_in, planes - 1, small_recv.at[2])
            shift = (first_slot - base)[0:1, 0:1]
            gap = (iota((window, block), 1) - iota((window, block), 0)).astype(F32)
            total = jnp.zeros((window, block), F32)
            for z in range(planes):
                total = total + jnp.where(gap + float(z * block) == shift, gates_in[z][0:1, :], 0.0)
            window_gate[...] = jnp.broadcast_to(
                jnp.sum(total, axis=1, keepdims=True), window_gate.shape
            )
        if step == 3:
            loads[3].wait()
            loads[4].wait()
            experts(2, 3)
        if step == 4:
            experts(0, 2)
    for c in every:
        ref = arrive(0, 5, c)
        if c in low:
            send(ref, 0, 6, c)
        final[at(5, c)] = ref[...]
        ref = arrive(1, 5, c)
        if c in high:
            send(ref, 1, 6, c)
        final[at(7, c)] = ref[...]
    experts(5, 2)
    for c in high:
        stage_right[1, :, columns(c)] = part[at(7, c)].astype(BF16)
        send_back(stage_right.at[1, :, columns(c)], 0, 2, c)
    for c in low:
        stage_left[1, :, columns(c)] = part[at(5, c)].astype(BF16)
        send_back(stage_left.at[1, :, columns(c)], 1, 2, c)
    for c in low:
        final[at(6, c)] = arrive(0, 6, c)[...]
    for c in high:
        final[at(6, c)] = arrive(1, 6, c)[...]
    experts(6, 1)
    for c in low:
        stage_right[0, :, columns(c)] = part[at(6, c)].astype(BF16)
        send_back(stage_right.at[0, :, columns(c)], 0, 1, c)
    for c in high:
        stage_left[0, :, columns(c)] = part[at(6, c)].astype(BF16)
        send_back(stage_left.at[0, :, columns(c)], 1, 1, c)
    for c in low:
        arrive_back(0, 1, c)
        stage_right[1, :, columns(c)] = (part[at(7, c)] + back_left[0, :, columns(c)].astype(F32)).astype(BF16)
        send_back(stage_right.at[1, :, columns(c)], 0, 2, c)
    for c in high:
        arrive_back(1, 1, c)
        stage_left[1, :, columns(c)] = (part[at(5, c)] + back_right[0, :, columns(c)].astype(F32)).astype(BF16)
        send_back(stage_left.at[1, :, columns(c)], 1, 2, c)

    def finish(k, c, total):
        rows = pl.ds((4 - k) * block, block)
        scaled[rows, columns(c)] = (window_gate[rows, 0:1] * total).astype(BF16)

    pick_table = table_of(
        target_column[:, 0:1] == iota((rows_all, window), 1).astype(F32)
    )
    for step in range(2, 7):
        for c in every:
            k = step - 2
            arrive_back(0, step, c)
            total = part[at(k, c)] + back_left[step - 1, :, columns(c)].astype(F32)
            if step < 6:
                stage_right[step, :, columns(c)] = total.astype(BF16)
                send_back(stage_right.at[step, :, columns(c)], 0, step + 1, c)
            if step == 5:
                finish(3, c, total + back_right[2, :, columns(c)].astype(F32))
            if step == 6:
                finish(4, c, total + back_right[1, :, columns(c)].astype(F32))
            k = 6 - step
            arrive_back(1, step, c)
            total = part[at(k, c)] + back_right[step - 1, :, columns(c)].astype(F32)
            if step < 6:
                stage_left[step, :, columns(c)] = total.astype(BF16)
                send_back(stage_left.at[step, :, columns(c)], 1, step + 1, c)
            if step == 4:
                finish(2, c, total + back_left[3, :, columns(c)].astype(F32))
            if step == 5:
                finish(1, c, total + back_left[2, :, columns(c)].astype(F32))
            if step == 6:
                finish(0, c, total + back_left[1, :, columns(c)].astype(F32))
                returned[:, :, columns(c)] = grouped(
                    dot(pick_table, scaled[:, columns(c)])
                ).astype(BF16)
                to_all_experts(
                    lambda peer: rows_of(returned, c).at[peer],
                    rows_of(results, c),
                    out_send.at[c],
                    out_recv.at[c],
                )
                results[my_expert, :, columns(c)] = returned[my_expert, :, columns(c)]
    for c in every:
        wait_all(rows_of(results, c), experts_all - 1, out_recv.at[c])
        out[:, columns(c)] = dot(
            take_table[...], flat(results[:, :, columns(c)]).astype(BF16)
        ).astype(out.dtype)

    for sent in started:
        sent.wait_send()
    wait_all(counts_out, experts_all - 1, small_send.at[0])
    wait_all(totals_in, planes - 1, small_send.at[1])
    wait_all(gates_in, planes - 1, small_send.at[2])
    for c in every:
        wait_all(rows_of(packed, c), experts_all - 1, rows_send.at[c])
        wait_all(rows_of(returned, c), experts_all - 1, out_send.at[c])


def on_device(tokens, expert_ranks, capacity, weight_in, weight_out, gate_weights):
    planes = lax.axis_size("dp")
    experts_all = lax.axis_size("expert")
    token_count, width = tokens.shape
    block = gate_weights.shape[1]
    units = weight_in.shape[2]
    rows_all = experts_all * MOST
    chunks = len(SIXTEENTHS)
    anywhere = pl.BlockSpec(memory_space=pl.ANY)
    slots = pltpu.VMEM((6, block, width), BF16)
    exchange = pltpu.VMEM((experts_all, MOST, width), BF16)
    ring_sems = pltpu.SemaphoreType.DMA((2, 6, chunks))
    chunk_sems = pltpu.SemaphoreType.DMA((chunks,))
    return pl.pallas_call(
        layer_kernel,
        out_shape=pltpu.VMEM((token_count, width), BF16),
        in_specs=[pl.BlockSpec(memory_space=pltpu.SMEM)] + [anywhere] * 5,
        out_specs=pl.BlockSpec(memory_space=pltpu.VMEM),
        scratch_shapes=[
            pltpu.VMEM(tokens.shape, BF16),
            pltpu.VMEM(expert_ranks.shape, jnp.int32),
            pltpu.VMEM(gate_weights.shape, F32),
            pltpu.VMEM(weight_in.shape[1:], BF16),
            pltpu.VMEM(weight_out.shape[1:], BF16),
            pltpu.VMEM((5, block, width), BF16),
            slots, slots,
            pltpu.VMEM((8 * block, width), BF16),
            pltpu.VMEM((3 * block, units), BF16),
            pltpu.VMEM((8 * block, width), F32),
            slots, slots, slots, slots,
            pltpu.VMEM((5 * block, width), BF16),
            exchange, exchange, exchange, exchange,
            pltpu.VMEM((experts_all, 1, LANES), F32),
            pltpu.VMEM((experts_all, 1, LANES), F32),
            pltpu.VMEM((experts_all, LANES), F32),
            pltpu.VMEM((MOST, LANES), F32),
            pltpu.VMEM((planes, MOST, LANES), F32),
            pltpu.VMEM((MOST, block), F32),
            pltpu.VMEM((planes, MOST, block), F32),
            pltpu.VMEM((5 * block, LANES), F32),
            pltpu.VMEM((5 * block, rows_all), BF16),
            pltpu.VMEM((rows_all, LANES), F32),
            pltpu.VMEM((token_count, rows_all), BF16),
            pltpu.SemaphoreType.DMA((5,)),
            ring_sems, ring_sems, ring_sems, ring_sems,
            chunk_sems, chunk_sems, chunk_sems, chunk_sems,
            pltpu.SemaphoreType.DMA((3,)),
            pltpu.SemaphoreType.DMA((3,)),
        ],
        compiler_params=pltpu.CompilerParams(
            collective_id=0, has_side_effects=True, vmem_limit_bytes=57 * 1024 * 1024
        ),
        name="layer",
    )(capacity, tokens, expert_ranks, gate_weights, weight_in[0], weight_out[0])


def solution(mesh):
    both = ("dp", "expert")
    placed = (
        P(both, None),
        P(None, both),
        P(),
        P("expert", None, "dp"),
        P("expert", "dp", None),
        P("expert", "dp"),
    )
    return jax.shard_map(
        on_device, mesh=mesh, in_specs=placed, out_specs=P(both, None), check_vma=False
    )
```

```python
import jax
import jax.numpy as jnp
from jax import lax
from jax.experimental import pallas as pl
from jax.experimental.pallas import tpu as pltpu
from jax.sharding import PartitionSpec as P

MOST = 8
SIXTEENTHS = (4, 4, 4, 4)
FIRST_HALF = 2
LANES = 128
PLACE_IN_F = {2: 0, 1: 1, 3: 2, 0: 3, 4: 4, 5: 5, 7: 6, 6: 7}
MESH_ID = pl.DeviceIdType.MESH
BF16 = jnp.bfloat16
F32 = jnp.float32


def iota(shape, dim):
    return lax.broadcasted_iota(jnp.int32, shape, dim)


def dot(a, b):
    return jnp.dot(a, b, preferred_element_type=F32)


def table_of(mask):
    return jnp.where(mask, 1.0, 0.0).astype(BF16)


def layer_kernel(
    capacity_hbm, tokens_hbm, ranks_hbm, gate_hbm, w_in_hbm, w_out_hbm, out,
    capacity, tokens, ranks, gate_in, w_in, w_out, own, from_left, from_right, final, hidden, part,
    back_left, back_right, stage_right, stage_left, scaled,
    packed, arrived, returned, results, counts_out, counts_in, counts_flat, totals_out, totals_in,
    gates_out, gates_in, window_gate, place_table, target_column, take_table,
    in_sem, send_sem, recv_sem, back_send_sem, back_recv_sem,
    rows_send, rows_recv, out_send, out_recv, small_send, small_recv,
):
    planes = lax.axis_size("dp")
    experts_all = lax.axis_size("expert")
    me = lax.axis_index("dp")
    my_expert = lax.axis_index("expert")
    right = lax.rem(me + 1, planes)
    left = lax.rem(me + planes - 1, planes)
    block = own.shape[1]
    width = own.shape[2]
    widths = [width // 16 * share for share in SIXTEENTHS]
    rows_all = experts_all * MOST
    window = 5 * block
    every = tuple(range(len(widths)))
    half = FIRST_HALF
    low, high = every[:half], every[half:]
    started = []

    loads = [
        pltpu.make_async_copy(src, dst, in_sem.at[n])
        for n, (src, dst) in enumerate(
            (
                (ranks_hbm, ranks),
                (gate_hbm, gate_in),
                (tokens_hbm, tokens),
                (w_in_hbm, w_in),
                (w_out_hbm, w_out),
                (capacity_hbm, capacity),
            )
        )
    ]
    for load in (loads[0], loads[5], loads[1], loads[2]):
        load.start()

    def partner(i):
        return lax.rem(my_expert + i + 1, experts_all)

    barrier = pltpu.get_barrier_semaphore()

    @pl.loop(0, experts_all - 1, unroll=True)
    def _(i):
        peer = partner(i)
        pl.semaphore_signal(barrier, inc=1, device_id={"expert": peer}, device_id_type=MESH_ID)

    @pl.loop(1, planes, unroll=True)
    def _(i):
        peer = lax.rem(me + i, planes)
        pl.semaphore_signal(barrier, inc=1, device_id={"dp": peer}, device_id_type=MESH_ID)

    def columns(c):
        return pl.ds(sum(widths[:c]), widths[c])

    def grouped(value):
        return value.reshape(experts_all, MOST, value.shape[-1])

    def flat(value):
        return value.astype(F32).reshape(rows_all, value.shape[-1])

    def to_all_experts(src_of, dst, sends, recvs):
        @pl.loop(0, experts_all - 1, unroll=True)
        def _(i):
            peer = partner(i)
            pltpu.make_async_remote_copy(
                src_ref=src_of(peer),
                dst_ref=dst.at[my_expert],
                send_sem=sends,
                recv_sem=recvs,
                device_id={"expert": peer},
                device_id_type=MESH_ID,
            ).start()

    def to_all_planes(src, dst, sends, recvs):
        @pl.loop(1, planes)
        def _(i):
            peer = lax.rem(me + i, planes)
            pltpu.make_async_remote_copy(
                src_ref=src,
                dst_ref=dst.at[me],
                send_sem=sends,
                recv_sem=recvs,
                device_id={"dp": peer},
                device_id_type=MESH_ID,
            ).start()

    def wait_all(ref, count, sem):
        several = ref.at[pl.ds(0, count)]
        pltpu.make_async_copy(several, several, sem).wait()

    def rows_of(ref, c):
        return ref.at[:, :, columns(c)]

    loads[5].wait()
    limits = jnp.zeros((experts_all, LANES), jnp.int32)
    for e in range(experts_all):
        limits = jnp.where(iota((experts_all, LANES), 0) == e, capacity[e], limits)
    token_count = tokens.shape[0]
    loads[0].wait()
    chosen = ranks[...] < limits[:, 0:1]
    chosen_table = table_of(chosen)
    taken = dot(chosen_table, jnp.ones((token_count, LANES), BF16))
    for e in range(experts_all):
        counts_out[e] = taken[e : e + 1, :]
    counts_in[my_expert] = counts_out[my_expert]
    loads[1].wait()
    gates_out[...] = jnp.broadcast_to(gate_in[...], gates_out.shape)
    gates_in[me] = gates_out[...]

    pl.semaphore_wait(barrier, experts_all + planes - 2)
    to_all_experts(lambda peer: counts_out.at[peer], counts_in, small_send.at[0], small_recv.at[0])
    to_all_planes(gates_out, gates_in, small_send.at[2], small_recv.at[2])

    earlier = table_of(iota((token_count, token_count), 0) < iota((token_count, token_count), 1))
    code = jnp.where(chosen, dot(chosen_table, earlier), -1.0).astype(BF16)
    expand = table_of(
        iota((rows_all, experts_all), 0) // MOST == iota((rows_all, experts_all), 1)
    )
    within = (iota((rows_all, token_count), 0) % MOST).astype(F32)
    pack = jnp.where(dot(expand, code) == within, 1.0, 0.0)
    pack_table = pack.astype(BF16)

    def pack_rows(c):
        packed[:, :, columns(c)] = grouped(dot(pack_table, tokens[:, columns(c)])).astype(BF16)
        to_all_experts(
            lambda peer: rows_of(packed, c).at[peer],
            rows_of(arrived, c),
            rows_send.at[c],
            rows_recv.at[c],
        )
        arrived[my_expert, :, columns(c)] = packed[my_expert, :, columns(c)]

    loads[2].wait()
    for load in loads[3:5]:
        load.start()
    pack_rows(0)
    pack_rows(1)

    wait_all(counts_in, experts_all - 1, small_recv.at[0])
    for e in range(experts_all):
        counts_flat[e : e + 1, :] = counts_in[e]
    counts = dot(expand, counts_flat[...].astype(BF16))
    totals_out[...] = jnp.broadcast_to(
        jnp.sum(counts_flat[...], axis=0, keepdims=True), totals_out.shape
    )
    to_all_planes(totals_out, totals_in, small_send.at[1], small_recv.at[1])
    totals_in[me] = totals_out[...]
    for c in every[2:]:
        pack_rows(c)
    counts_table = counts.astype(BF16)
    row_ids = iota((rows_all, rows_all), 0)
    lane_ids = iota((rows_all, rows_all), 1)
    ahead = jnp.logical_and(lane_ids % MOST == 0, lane_ids // MOST < row_ids // MOST)
    starts = dot(table_of(ahead), counts_table)
    place_in = (iota((rows_all, LANES), 0) % MOST).astype(F32)
    take_table[...] = pack.T.astype(BF16)
    taken_row = jnp.where(place_in < counts, 1.0, 0.0).T[0:1, :] > 0.5
    place_row = (starts + place_in).T[0:1, :]
    wait_all(totals_in, planes - 1, small_recv.at[1])
    plane_counts = [totals_in[z] for z in range(planes)]
    left_over = jnp.full((MOST, LANES), float(planes * block), F32)
    for z in range(planes):
        left_over = left_over - plane_counts[z]
    padded_start = jnp.zeros((MOST, LANES), F32)
    first_slot = padded_start
    drift_mine = padded_start
    drift_most = padded_start
    for z in range(planes):
        drift = padded_start - float(z * block)
        drift_most = jnp.maximum(drift_most, drift)
        drift_mine = jnp.where(me == z, drift, drift_mine)
        first_slot = first_slot + jnp.where(me > z, plane_counts[z], 0.0)
        extra = jnp.minimum(2.0 * block - plane_counts[z], left_over)
        left_over = left_over - extra
        padded_start = padded_start + plane_counts[z] + extra
    base = drift_mine - drift_most + 4.0 * block
    target_row = jnp.where(taken_row, base[0:1, 0:1] + place_row, -1.0)
    place_table[...] = table_of(target_row == iota((window, rows_all), 0).astype(F32))
    target_column[...] = jnp.where(place_in < counts, base[0:1, :] + starts + place_in, -1.0)

    def copy(src, dst, sends, recvs, way, step, c):
        return pltpu.make_async_remote_copy(
            src_ref=src,
            dst_ref=dst.at[step - 1, :, columns(c)],
            send_sem=sends.at[way, step - 1, c],
            recv_sem=recvs.at[way, step - 1, c],
            device_id={"dp": right if way == 0 else left},
            device_id_type=MESH_ID,
        )

    def send(src, way, step, c):
        sent = copy(src, from_left if way == 0 else from_right, send_sem, recv_sem, way, step, c)
        sent.start()
        started.append(sent)

    def arrive(way, step, c):
        into = from_left if way == 0 else from_right
        ref = into.at[step - 1, :, columns(c)]
        copy(ref, into, send_sem, recv_sem, way, step, c).wait_recv()
        return ref

    def send_back(src, way, step, c):
        sent = copy(
            src, back_left if way == 0 else back_right, back_send_sem, back_recv_sem, way, step, c
        )
        sent.start()
        started.append(sent)

    def arrive_back(way, step, c):
        into = back_left if way == 0 else back_right
        ref = into.at[step - 1, :, columns(c)]
        copy(ref, into, back_send_sem, back_recv_sem, way, step, c).wait_recv()

    def at(k, c):
        return pl.ds(PLACE_IN_F[k] * block, block), columns(c)

    def place(k, c, rows):
        own[k, :, columns(c)] = dot(place_table[pl.ds((4 - k) * block, block), :], rows).astype(BF16)

    def arrived_rows(c):
        return flat(arrived[:, :, columns(c)]).astype(BF16)

    for c in every:
        wait_all(rows_of(arrived, c), experts_all - 1, rows_recv.at[c])
        rows = arrived_rows(c)
        place(0, c, rows)
        send(own.at[0, :, columns(c)], 0, 1, c)
        place(4, c, rows)
        send(own.at[4, :, columns(c)], 1, 1, c)
        for k in (1, 3, 2):
            place(k, c, rows)

    def experts(low_k, count):
        row = PLACE_IN_F[low_k] * block
        rows = count * block
        tile = min(256, w_in.shape[1])

        @pl.loop(0, w_in.shape[1] // tile)
        def _(n):
            at_n = pl.ds(pl.multiple_of(n * tile, tile), tile)
            total = dot(final[pl.ds(row, rows), :], w_in[:, at_n])
            hidden[pl.ds(0, rows), at_n] = jnp.maximum(total, 0.0).astype(BF16)

        @pl.loop(0, w_out.shape[1] // tile)
        def _(n):
            at_n = pl.ds(pl.multiple_of(n * tile, tile), tile)
            part[pl.ds(row, rows), at_n] = dot(hidden[pl.ds(0, rows), :], w_out[:, at_n])

    for step in range(1, 5):
        for c in every:
            ref = arrive(0, step, c)
            value = ref[...]
            total = value + own[step, :, columns(c)]
            ref[...] = total
            send(ref, 0, step + 1, c)
            if step == 3:
                final[at(3, c)] = value + from_right[0, :, columns(c)]
            if step == 4:
                final[at(4, c)] = total
            ref = arrive(1, step, c)
            value = ref[...]
            total = value + own[4 - step, :, columns(c)]
            ref[...] = total
            send(ref, 1, step + 1, c)
            if step == 2:
                final[at(2, c)] = value + from_left[1, :, columns(c)]
            if step == 3:
                final[at(1, c)] = value + from_left[0, :, columns(c)]
            if step == 4:
                final[at(0, c)] = total
        if step == 1:
            wait_all(gates_in, planes - 1, small_recv.at[2])
            shift = (first_slot - base)[0:1, 0:1]
            gap = (iota((window, block), 1) - iota((window, block), 0)).astype(F32)
            total = jnp.zeros((window, block), F32)
            for z in range(planes):
                total = total + jnp.where(gap + float(z * block) == shift, gates_in[z][0:1, :], 0.0)
            window_gate[...] = jnp.broadcast_to(
                jnp.sum(total, axis=1, keepdims=True), window_gate.shape
            )
        if step == 3:
            loads[3].wait()
            loads[4].wait()
            experts(2, 3)
        if step == 4:
            experts(0, 2)
    for c in every:
        ref = arrive(0, 5, c)
        if c in low:
            send(ref, 0, 6, c)
        final[at(5, c)] = ref[...]
        ref = arrive(1, 5, c)
        if c in high:
            send(ref, 1, 6, c)
        final[at(7, c)] = ref[...]
    experts(5, 2)
    for c in high:
        stage_right[1, :, columns(c)] = part[at(7, c)].astype(BF16)
        send_back(stage_right.at[1, :, columns(c)], 0, 2, c)
    for c in low:
        stage_left[1, :, columns(c)] = part[at(5, c)].astype(BF16)
        send_back(stage_left.at[1, :, columns(c)], 1, 2, c)
    for c in low:
        final[at(6, c)] = arrive(0, 6, c)[...]
    for c in high:
        final[at(6, c)] = arrive(1, 6, c)[...]
    experts(6, 1)
    for c in low:
        stage_right[0, :, columns(c)] = part[at(6, c)].astype(BF16)
        send_back(stage_right.at[0, :, columns(c)], 0, 1, c)
    for c in high:
        stage_left[0, :, columns(c)] = part[at(6, c)].astype(BF16)
        send_back(stage_left.at[0, :, columns(c)], 1, 1, c)
    for c in low:
        arrive_back(0, 1, c)
        stage_right[1, :, columns(c)] = (part[at(7, c)] + back_left[0, :, columns(c)].astype(F32)).astype(BF16)
        send_back(stage_right.at[1, :, columns(c)], 0, 2, c)
    for c in high:
        arrive_back(1, 1, c)
        stage_left[1, :, columns(c)] = (part[at(5, c)] + back_right[0, :, columns(c)].astype(F32)).astype(BF16)
        send_back(stage_left.at[1, :, columns(c)], 1, 2, c)

    def finish(k, c, total):
        rows = pl.ds((4 - k) * block, block)
        scaled[rows, columns(c)] = (window_gate[rows, 0:1] * total).astype(BF16)

    pick_table = table_of(
        target_column[:, 0:1] == iota((rows_all, window), 1).astype(F32)
    )
    for step in range(2, 7):
        for c in every:
            k = step - 2
            arrive_back(0, step, c)
            total = part[at(k, c)] + back_left[step - 1, :, columns(c)].astype(F32)
            if step < 6:
                stage_right[step, :, columns(c)] = total.astype(BF16)
                send_back(stage_right.at[step, :, columns(c)], 0, step + 1, c)
            if step == 5:
                finish(3, c, total + back_right[2, :, columns(c)].astype(F32))
            if step == 6:
                finish(4, c, total + back_right[1, :, columns(c)].astype(F32))
            k = 6 - step
            arrive_back(1, step, c)
            total = part[at(k, c)] + back_right[step - 1, :, columns(c)].astype(F32)
            if step < 6:
                stage_left[step, :, columns(c)] = total.astype(BF16)
                send_back(stage_left.at[step, :, columns(c)], 1, step + 1, c)
            if step == 4:
                finish(2, c, total + back_left[3, :, columns(c)].astype(F32))
            if step == 5:
                finish(1, c, total + back_left[2, :, columns(c)].astype(F32))
            if step == 6:
                finish(0, c, total + back_left[1, :, columns(c)].astype(F32))
                returned[:, :, columns(c)] = grouped(
                    dot(pick_table, scaled[:, columns(c)])
                ).astype(BF16)
                to_all_experts(
                    lambda peer: rows_of(returned, c).at[peer],
                    rows_of(results, c),
                    out_send.at[c],
                    out_recv.at[c],
                )
                results[my_expert, :, columns(c)] = returned[my_expert, :, columns(c)]
    for sent in started:
        sent.wait_send()
    wait_all(counts_out, experts_all - 1, small_send.at[0])
    wait_all(totals_in, planes - 1, small_send.at[1])
    wait_all(gates_in, planes - 1, small_send.at[2])
    for c in every:
        wait_all(rows_of(packed, c), experts_all - 1, rows_send.at[c])
    for c in every:
        wait_all(rows_of(results, c), experts_all - 1, out_recv.at[c])
        out[:, columns(c)] = dot(
            take_table[...], flat(results[:, :, columns(c)]).astype(BF16)
        ).astype(out.dtype)

    for c in every:
        wait_all(rows_of(returned, c), experts_all - 1, out_send.at[c])


def on_device(tokens, expert_ranks, capacity, weight_in, weight_out, gate_weights):
    planes = lax.axis_size("dp")
    experts_all = lax.axis_size("expert")
    token_count, width = tokens.shape
    block = gate_weights.shape[1]
    units = weight_in.shape[2]
    rows_all = experts_all * MOST
    chunks = len(SIXTEENTHS)
    anywhere = pl.BlockSpec(memory_space=pl.ANY)
    slots = pltpu.VMEM((6, block, width), BF16)
    exchange = pltpu.VMEM((experts_all, MOST, width), BF16)
    ring_sems = pltpu.SemaphoreType.DMA((2, 6, chunks))
    chunk_sems = pltpu.SemaphoreType.DMA((chunks,))
    return pl.pallas_call(
        layer_kernel,
        out_shape=pltpu.VMEM((token_count, width), BF16),
        in_specs=[anywhere] * 6,
        out_specs=pl.BlockSpec(memory_space=pltpu.VMEM),
        scratch_shapes=[
            pltpu.SMEM(capacity.shape, jnp.int32),
            pltpu.VMEM(tokens.shape, BF16),
            pltpu.VMEM(expert_ranks.shape, jnp.int32),
            pltpu.VMEM(gate_weights.shape, F32),
            pltpu.VMEM(weight_in.shape[1:], BF16),
            pltpu.VMEM(weight_out.shape[1:], BF16),
            pltpu.VMEM((5, block, width), BF16),
            slots, slots,
            pltpu.VMEM((8 * block, width), BF16),
            pltpu.VMEM((3 * block, units), BF16),
            pltpu.VMEM((8 * block, width), F32),
            slots, slots, slots, slots,
            pltpu.VMEM((5 * block, width), BF16),
            exchange, exchange, exchange, exchange,
            pltpu.VMEM((experts_all, 1, LANES), F32),
            pltpu.VMEM((experts_all, 1, LANES), F32),
            pltpu.VMEM((experts_all, LANES), F32),
            pltpu.VMEM((MOST, LANES), F32),
            pltpu.VMEM((planes, MOST, LANES), F32),
            pltpu.VMEM((MOST, block), F32),
            pltpu.VMEM((planes, MOST, block), F32),
            pltpu.VMEM((5 * block, LANES), F32),
            pltpu.VMEM((5 * block, rows_all), BF16),
            pltpu.VMEM((rows_all, LANES), F32),
            pltpu.VMEM((token_count, rows_all), BF16),
            pltpu.SemaphoreType.DMA((6,)),
            ring_sems, ring_sems, ring_sems, ring_sems,
            chunk_sems, chunk_sems, chunk_sems, chunk_sems,
            pltpu.SemaphoreType.DMA((3,)),
            pltpu.SemaphoreType.DMA((3,)),
        ],
        compiler_params=pltpu.CompilerParams(
            collective_id=0, has_side_effects=True, vmem_limit_bytes=57 * 1024 * 1024
        ),
        name="layer",
    )(capacity, tokens, expert_ranks, gate_weights, weight_in[0], weight_out[0])


def solution(mesh):
    both = ("dp", "expert")
    placed = (
        P(both, None),
        P(None, both),
        P(),
        P("expert", None, "dp"),
        P("expert", "dp", None),
        P("expert", "dp"),
    )
    return jax.shard_map(
        on_device, mesh=mesh, in_specs=placed, out_specs=P(both, None), check_vma=False
    )
```

```python
import jax
import jax.numpy as jnp
from jax import lax
from jax.experimental import pallas as pl
from jax.experimental.pallas import tpu as pltpu
from jax.sharding import PartitionSpec as P

MOST = 8
SIXTEENTHS = (4, 4, 4, 4)
FIRST_HALF = 2
LANES = 128
PLACE_IN_F = {2: 0, 1: 1, 3: 2, 0: 3, 4: 4, 5: 5, 7: 6, 6: 7}
MESH_ID = pl.DeviceIdType.MESH
BF16 = jnp.bfloat16
F32 = jnp.float32


def iota(shape, dim):
    return lax.broadcasted_iota(jnp.int32, shape, dim)


def dot(a, b):
    return jnp.dot(a, b, preferred_element_type=F32)


def table_of(mask):
    return jnp.where(mask, 1.0, 0.0).astype(BF16)


def layer_kernel(
    capacity_hbm, tokens_hbm, ranks_hbm, gate_hbm, w_in_hbm, w_out_hbm, out,
    capacity, tokens, ranks, gate_in, w_in, w_out, own, from_left, from_right, final, hidden, part,
    back_left, back_right, stage_right, stage_left, scaled,
    packed, arrived, returned, results, counts_out, counts_in, counts_flat, totals_out, totals_in,
    gates_out, gates_in, window_gate, place_table, target_column, take_table, first_rows,
    in_sem, send_sem, recv_sem, back_send_sem, back_recv_sem,
    rows_send, rows_recv, out_send, out_recv, small_send, small_recv,
):
    planes = lax.axis_size("dp")
    experts_all = lax.axis_size("expert")
    me = lax.axis_index("dp")
    my_expert = lax.axis_index("expert")
    right = lax.rem(me + 1, planes)
    left = lax.rem(me + planes - 1, planes)
    block = own.shape[1]
    width = own.shape[2]
    widths = [width // 16 * share for share in SIXTEENTHS]
    rows_all = experts_all * MOST
    window = 5 * block
    every = tuple(range(len(widths)))
    half = FIRST_HALF
    low, high = every[:half], every[half:]
    started = []

    loads = [
        pltpu.make_async_copy(src, dst, in_sem.at[n])
        for n, (src, dst) in enumerate(
            (
                (ranks_hbm, ranks),
                (gate_hbm, gate_in),
                (tokens_hbm, tokens),
                (w_in_hbm, w_in),
                (w_out_hbm, w_out),
                (capacity_hbm, capacity),
            )
        )
    ]
    for load in (loads[0], loads[5], loads[1], loads[2]):
        load.start()

    def partner(i):
        return lax.rem(my_expert + i + 1, experts_all)

    barrier = pltpu.get_barrier_semaphore()

    @pl.loop(0, experts_all - 1, unroll=True)
    def _(i):
        peer = partner(i)
        pl.semaphore_signal(barrier, inc=1, device_id={"expert": peer}, device_id_type=MESH_ID)

    @pl.loop(1, planes, unroll=True)
    def _(i):
        peer = lax.rem(me + i, planes)
        pl.semaphore_signal(barrier, inc=1, device_id={"dp": peer}, device_id_type=MESH_ID)

    def columns(c):
        return pl.ds(sum(widths[:c]), widths[c])

    def grouped(value):
        return value.reshape(experts_all, MOST, value.shape[-1])

    def flat(value):
        return value.astype(F32).reshape(rows_all, value.shape[-1])

    def to_all_experts(src_of, dst, sends, recvs):
        @pl.loop(0, experts_all - 1, unroll=True)
        def _(i):
            peer = partner(i)
            pltpu.make_async_remote_copy(
                src_ref=src_of(peer),
                dst_ref=dst.at[my_expert],
                send_sem=sends,
                recv_sem=recvs,
                device_id={"expert": peer},
                device_id_type=MESH_ID,
            ).start()

    def to_all_planes(src, dst, sends, recvs):
        @pl.loop(1, planes)
        def _(i):
            peer = lax.rem(me + i, planes)
            pltpu.make_async_remote_copy(
                src_ref=src,
                dst_ref=dst.at[me],
                send_sem=sends,
                recv_sem=recvs,
                device_id={"dp": peer},
                device_id_type=MESH_ID,
            ).start()

    def wait_all(ref, count, sem):
        several = ref.at[pl.ds(0, count)]
        pltpu.make_async_copy(several, several, sem).wait()

    def rows_of(ref, c):
        return ref.at[:, :, columns(c)]

    loads[5].wait()
    limits = jnp.zeros((experts_all, LANES), jnp.int32)
    for e in range(experts_all):
        limits = jnp.where(iota((experts_all, LANES), 0) == e, capacity[e], limits)
    token_count = tokens.shape[0]
    loads[0].wait()
    chosen = ranks[...] < limits[:, 0:1]
    chosen_table = table_of(chosen)
    taken = dot(chosen_table, jnp.ones((token_count, LANES), BF16))
    for e in range(experts_all):
        counts_out[e] = taken[e : e + 1, :]
    counts_in[my_expert] = counts_out[my_expert]

    pl.semaphore_wait(barrier, experts_all + planes - 2)
    to_all_experts(lambda peer: counts_out.at[peer], counts_in, small_send.at[0], small_recv.at[0])

    earlier = table_of(iota((token_count, token_count), 0) < iota((token_count, token_count), 1))
    code = jnp.where(chosen, dot(chosen_table, earlier), -1.0).astype(BF16)
    expand = table_of(
        iota((rows_all, experts_all), 0) // MOST == iota((rows_all, experts_all), 1)
    )
    within = (iota((rows_all, token_count), 0) % MOST).astype(F32)
    pack = jnp.where(dot(expand, code) == within, 1.0, 0.0)
    pack_table = pack.astype(BF16)

    def pack_rows(c):
        packed[:, :, columns(c)] = grouped(dot(pack_table, tokens[:, columns(c)])).astype(BF16)
        to_all_experts(
            lambda peer: rows_of(packed, c).at[peer],
            rows_of(arrived, c),
            rows_send.at[c],
            rows_recv.at[c],
        )
        arrived[my_expert, :, columns(c)] = packed[my_expert, :, columns(c)]

    loads[2].wait()
    for load in loads[3:5]:
        load.start()
    pack_rows(0)
    pack_rows(1)

    wait_all(counts_in, experts_all - 1, small_recv.at[0])
    for e in range(experts_all):
        counts_flat[e : e + 1, :] = counts_in[e]
    counts = dot(expand, counts_flat[...].astype(BF16))
    totals_out[...] = jnp.broadcast_to(
        jnp.sum(counts_flat[...], axis=0, keepdims=True), totals_out.shape
    )
    to_all_planes(totals_out, totals_in, small_send.at[1], small_recv.at[1])
    totals_in[me] = totals_out[...]
    for c in every[2:]:
        pack_rows(c)
    loads[1].wait()
    gates_out[...] = jnp.broadcast_to(gate_in[...], gates_out.shape)
    gates_in[me] = gates_out[...]
    to_all_planes(gates_out, gates_in, small_send.at[2], small_recv.at[2])
    counts_table = counts.astype(BF16)
    row_ids = iota((rows_all, rows_all), 0)
    lane_ids = iota((rows_all, rows_all), 1)
    ahead = jnp.logical_and(lane_ids % MOST == 0, lane_ids // MOST < row_ids // MOST)
    starts = dot(table_of(ahead), counts_table)
    place_in = (iota((rows_all, LANES), 0) % MOST).astype(F32)
    take_table[...] = pack.T.astype(BF16)
    taken_row = jnp.where(place_in < counts, 1.0, 0.0).T[0:1, :] > 0.5
    place_row = (starts + place_in).T[0:1, :]
    wait_all(rows_of(arrived, 0), experts_all - 1, rows_recv.at[0])
    first_rows[...] = flat(arrived[:, :, columns(0)]).astype(BF16)
    wait_all(totals_in, planes - 1, small_recv.at[1])
    plane_counts = [totals_in[z] for z in range(planes)]
    left_over = jnp.full((MOST, LANES), float(planes * block), F32)
    for z in range(planes):
        left_over = left_over - plane_counts[z]
    padded_start = jnp.zeros((MOST, LANES), F32)
    first_slot = padded_start
    drift_mine = padded_start
    drift_most = padded_start
    for z in range(planes):
        drift = padded_start - float(z * block)
        drift_most = jnp.maximum(drift_most, drift)
        drift_mine = jnp.where(me == z, drift, drift_mine)
        first_slot = first_slot + jnp.where(me > z, plane_counts[z], 0.0)
        extra = jnp.minimum(2.0 * block - plane_counts[z], left_over)
        left_over = left_over - extra
        padded_start = padded_start + plane_counts[z] + extra
    base = drift_mine - drift_most + 4.0 * block
    target_row = jnp.where(taken_row, base[0:1, 0:1] + place_row, -1.0)
    place_table[...] = table_of(target_row == iota((window, rows_all), 0).astype(F32))
    target_column[...] = jnp.where(place_in < counts, base[0:1, :] + starts + place_in, -1.0)

    def copy(src, dst, sends, recvs, way, step, c):
        return pltpu.make_async_remote_copy(
            src_ref=src,
            dst_ref=dst.at[step - 1, :, columns(c)],
            send_sem=sends.at[way, step - 1, c],
            recv_sem=recvs.at[way, step - 1, c],
            device_id={"dp": right if way == 0 else left},
            device_id_type=MESH_ID,
        )

    def send(src, way, step, c):
        sent = copy(src, from_left if way == 0 else from_right, send_sem, recv_sem, way, step, c)
        sent.start()
        started.append(sent)

    def arrive(way, step, c):
        into = from_left if way == 0 else from_right
        ref = into.at[step - 1, :, columns(c)]
        copy(ref, into, send_sem, recv_sem, way, step, c).wait_recv()
        return ref

    def send_back(src, way, step, c):
        sent = copy(
            src, back_left if way == 0 else back_right, back_send_sem, back_recv_sem, way, step, c
        )
        sent.start()
        started.append(sent)

    def arrive_back(way, step, c):
        into = back_left if way == 0 else back_right
        ref = into.at[step - 1, :, columns(c)]
        copy(ref, into, back_send_sem, back_recv_sem, way, step, c).wait_recv()

    def at(k, c):
        return pl.ds(PLACE_IN_F[k] * block, block), columns(c)

    def place(k, c, rows):
        own[k, :, columns(c)] = dot(place_table[pl.ds((4 - k) * block, block), :], rows).astype(BF16)

    def arrived_rows(c):
        return flat(arrived[:, :, columns(c)]).astype(BF16)

    for c in every:
        if c == 0:
            rows = first_rows[...]
        else:
            wait_all(rows_of(arrived, c), experts_all - 1, rows_recv.at[c])
            rows = arrived_rows(c)
        place(0, c, rows)
        send(own.at[0, :, columns(c)], 0, 1, c)
        place(4, c, rows)
        send(own.at[4, :, columns(c)], 1, 1, c)
        for k in (1, 3, 2):
            place(k, c, rows)

    def experts(low_k, count):
        row = PLACE_IN_F[low_k] * block
        rows = count * block
        tile = min(256, w_in.shape[1])

        @pl.loop(0, w_in.shape[1] // tile)
        def _(n):
            at_n = pl.ds(pl.multiple_of(n * tile, tile), tile)
            total = dot(final[pl.ds(row, rows), :], w_in[:, at_n])
            hidden[pl.ds(0, rows), at_n] = jnp.maximum(total, 0.0).astype(BF16)

        @pl.loop(0, w_out.shape[1] // tile)
        def _(n):
            at_n = pl.ds(pl.multiple_of(n * tile, tile), tile)
            part[pl.ds(row, rows), at_n] = dot(hidden[pl.ds(0, rows), :], w_out[:, at_n])

    for step in range(1, 5):
        for c in every:
            ref = arrive(0, step, c)
            value = ref[...]
            total = value + own[step, :, columns(c)]
            ref[...] = total
            send(ref, 0, step + 1, c)
            if step == 3:
                final[at(3, c)] = value + from_right[0, :, columns(c)]
            if step == 4:
                final[at(4, c)] = total
            ref = arrive(1, step, c)
            value = ref[...]
            total = value + own[4 - step, :, columns(c)]
            ref[...] = total
            send(ref, 1, step + 1, c)
            if step == 2:
                final[at(2, c)] = value + from_left[1, :, columns(c)]
            if step == 3:
                final[at(1, c)] = value + from_left[0, :, columns(c)]
            if step == 4:
                final[at(0, c)] = total
        if step == 1:
            wait_all(gates_in, planes - 1, small_recv.at[2])
            shift = (first_slot - base)[0:1, 0:1]
            gap = (iota((window, block), 1) - iota((window, block), 0)).astype(F32)
            total = jnp.zeros((window, block), F32)
            for z in range(planes):
                total = total + jnp.where(gap + float(z * block) == shift, gates_in[z][0:1, :], 0.0)
            window_gate[...] = jnp.broadcast_to(
                jnp.sum(total, axis=1, keepdims=True), window_gate.shape
            )
        if step == 3:
            loads[3].wait()
            loads[4].wait()
            experts(2, 3)
        if step == 4:
            experts(0, 2)
    for c in every:
        ref = arrive(0, 5, c)
        if c in low:
            send(ref, 0, 6, c)
        final[at(5, c)] = ref[...]
        ref = arrive(1, 5, c)
        if c in high:
            send(ref, 1, 6, c)
        final[at(7, c)] = ref[...]
    experts(5, 2)
    for c in high:
        stage_right[1, :, columns(c)] = part[at(7, c)].astype(BF16)
        send_back(stage_right.at[1, :, columns(c)], 0, 2, c)
    for c in low:
        stage_left[1, :, columns(c)] = part[at(5, c)].astype(BF16)
        send_back(stage_left.at[1, :, columns(c)], 1, 2, c)
    for c in low:
        final[at(6, c)] = arrive(0, 6, c)[...]
    for c in high:
        final[at(6, c)] = arrive(1, 6, c)[...]
    experts(6, 1)
    for c in low:
        stage_right[0, :, columns(c)] = part[at(6, c)].astype(BF16)
        send_back(stage_right.at[0, :, columns(c)], 0, 1, c)
    for c in high:
        stage_left[0, :, columns(c)] = part[at(6, c)].astype(BF16)
        send_back(stage_left.at[0, :, columns(c)], 1, 1, c)
    for c in low:
        arrive_back(0, 1, c)
        stage_right[1, :, columns(c)] = (part[at(7, c)] + back_left[0, :, columns(c)].astype(F32)).astype(BF16)
        send_back(stage_right.at[1, :, columns(c)], 0, 2, c)
    for c in high:
        arrive_back(1, 1, c)
        stage_left[1, :, columns(c)] = (part[at(5, c)] + back_right[0, :, columns(c)].astype(F32)).astype(BF16)
        send_back(stage_left.at[1, :, columns(c)], 1, 2, c)

    def finish(k, c, total):
        rows = pl.ds((4 - k) * block, block)
        scaled[rows, columns(c)] = (window_gate[rows, 0:1] * total).astype(BF16)

    pick_table = table_of(
        target_column[:, 0:1] == iota((rows_all, window), 1).astype(F32)
    )
    for step in range(2, 7):
        for c in every:
            k = step - 2
            arrive_back(0, step, c)
            total = part[at(k, c)] + back_left[step - 1, :, columns(c)].astype(F32)
            if step < 6:
                stage_right[step, :, columns(c)] = total.astype(BF16)
                send_back(stage_right.at[step, :, columns(c)], 0, step + 1, c)
            if step == 5:
                finish(3, c, total + back_right[2, :, columns(c)].astype(F32))
            if step == 6:
                finish(4, c, total + back_right[1, :, columns(c)].astype(F32))
            k = 6 - step
            arrive_back(1, step, c)
            total = part[at(k, c)] + back_right[step - 1, :, columns(c)].astype(F32)
            if step < 6:
                stage_left[step, :, columns(c)] = total.astype(BF16)
                send_back(stage_left.at[step, :, columns(c)], 1, step + 1, c)
            if step == 4:
                finish(2, c, total + back_left[3, :, columns(c)].astype(F32))
            if step == 5:
                finish(1, c, total + back_left[2, :, columns(c)].astype(F32))
            if step == 6:
                finish(0, c, total + back_left[1, :, columns(c)].astype(F32))
                returned[:, :, columns(c)] = grouped(
                    dot(pick_table, scaled[:, columns(c)])
                ).astype(BF16)
                to_all_experts(
                    lambda peer: rows_of(returned, c).at[peer],
                    rows_of(results, c),
                    out_send.at[c],
                    out_recv.at[c],
                )
                results[my_expert, :, columns(c)] = returned[my_expert, :, columns(c)]
    for sent in started:
        sent.wait_send()
    wait_all(counts_out, experts_all - 1, small_send.at[0])
    wait_all(totals_in, planes - 1, small_send.at[1])
    wait_all(gates_in, planes - 1, small_send.at[2])
    for c in every:
        wait_all(rows_of(packed, c), experts_all - 1, rows_send.at[c])
    for c in every:
        wait_all(rows_of(results, c), experts_all - 1, out_recv.at[c])
        out[:, columns(c)] = dot(
            take_table[...], flat(results[:, :, columns(c)]).astype(BF16)
        ).astype(out.dtype)

    for c in every:
        wait_all(rows_of(returned, c), experts_all - 1, out_send.at[c])


def on_device(tokens, expert_ranks, capacity, weight_in, weight_out, gate_weights):
    planes = lax.axis_size("dp")
    experts_all = lax.axis_size("expert")
    token_count, width = tokens.shape
    block = gate_weights.shape[1]
    units = weight_in.shape[2]
    rows_all = experts_all * MOST
    chunks = len(SIXTEENTHS)
    anywhere = pl.BlockSpec(memory_space=pl.ANY)
    slots = pltpu.VMEM((6, block, width), BF16)
    exchange = pltpu.VMEM((experts_all, MOST, width), BF16)
    ring_sems = pltpu.SemaphoreType.DMA((2, 6, chunks))
    chunk_sems = pltpu.SemaphoreType.DMA((chunks,))
    return pl.pallas_call(
        layer_kernel,
        out_shape=pltpu.VMEM((token_count, width), BF16),
        in_specs=[anywhere] * 6,
        out_specs=pl.BlockSpec(memory_space=pltpu.VMEM),
        scratch_shapes=[
            pltpu.SMEM(capacity.shape, jnp.int32),
            pltpu.VMEM(tokens.shape, BF16),
            pltpu.VMEM(expert_ranks.shape, jnp.int32),
            pltpu.VMEM(gate_weights.shape, F32),
            pltpu.VMEM(weight_in.shape[1:], BF16),
            pltpu.VMEM(weight_out.shape[1:], BF16),
            pltpu.VMEM((5, block, width), BF16),
            slots, slots,
            pltpu.VMEM((8 * block, width), BF16),
            pltpu.VMEM((3 * block, units), BF16),
            pltpu.VMEM((8 * block, width), F32),
            slots, slots, slots, slots,
            pltpu.VMEM((5 * block, width), BF16),
            exchange, exchange, exchange, exchange,
            pltpu.VMEM((experts_all, 1, LANES), F32),
            pltpu.VMEM((experts_all, 1, LANES), F32),
            pltpu.VMEM((experts_all, LANES), F32),
            pltpu.VMEM((MOST, LANES), F32),
            pltpu.VMEM((planes, MOST, LANES), F32),
            pltpu.VMEM((MOST, block), F32),
            pltpu.VMEM((planes, MOST, block), F32),
            pltpu.VMEM((5 * block, LANES), F32),
            pltpu.VMEM((5 * block, rows_all), BF16),
            pltpu.VMEM((rows_all, LANES), F32),
            pltpu.VMEM((token_count, rows_all), BF16),
            pltpu.VMEM((rows_all, width // 16 * SIXTEENTHS[0]), BF16),
            pltpu.SemaphoreType.DMA((6,)),
            ring_sems, ring_sems, ring_sems, ring_sems,
            chunk_sems, chunk_sems, chunk_sems, chunk_sems,
            pltpu.SemaphoreType.DMA((3,)),
            pltpu.SemaphoreType.DMA((3,)),
        ],
        compiler_params=pltpu.CompilerParams(
            collective_id=0, has_side_effects=True, vmem_limit_bytes=57 * 1024 * 1024
        ),
        name="layer",
    )(capacity, tokens, expert_ranks, gate_weights, weight_in[0], weight_out[0])


def solution(mesh):
    both = ("dp", "expert")
    placed = (
        P(both, None),
        P(None, both),
        P(),
        P("expert", None, "dp"),
        P("expert", "dp", None),
        P("expert", "dp"),
    )
    return jax.shard_map(
        on_device, mesh=mesh, in_specs=placed, out_specs=P(both, None), check_vma=False
    )
```
